256 devices in a mesh: leaf: 32 (over z, x), rows: 8 (over y, core).
Axes of the slice: x: 4, y: 4, z: 8, core: 2. Of those that a mesh axis runs over, the one named last changes fastest.
Arguments:
- right_side: float32 [8, 262144], P(None, ('leaf', 'rows')), may hold values from -6 to 6
- diagonal: float32 [262144], P(('leaf', 'rows')), may hold values from 0.5 to 4
- tree_order: int32 [262144], P(('leaf', 'rows')), may hold values from 0 to 262143, as said below
- mid_perm: int32 [32], replicated, may hold values from 0 to 31, each once
- col_factor: bfloat16 [262144, 1536], P(('leaf', 'rows')), may hold values from -0.1875 to 0.1875
- mid_factor: bfloat16 [49152, 3072], P('leaf', 'rows'), may hold values from -0.0546875 to 0.0546875
- pre_factor: bfloat16 [49152, 3072], P('leaf', 'rows'), may hold values from -0.0546875 to 0.0546875
- row_factor: bfloat16 [48, 262144], P(None, ('leaf', 'rows')), may hold values from -0.875 to 0.875
Outputs:
- solution: float32 [8, 262144], P(None, ('leaf', 'rows'))
- residual: float32 [8, 262144], P(None, ('leaf', 'rows'))
The draws below stay inside these ranges and needn't reach their ends.
Inputs may be any that keep to these rules, and one draw needn't show every extreme that they name: `tree_order`: each aligned run of 1024 entries, the run starting at b * 1024, is a permutation of b * 1024 to (b + 1) * 1024 - 1. `mid_perm`: a permutation of 0 to 31.
All inputs are finite; a program needn't handle non-finite values.
Results may differ from the reference program's by a relative error of at most 0.025.
Values may be sent and summed in bfloat16 or wider, within the bound.
A program may use at most 64 MiB of HBM per device.

```python
import math
import jax
import jax.numpy as jnp
from jax import lax

PTS = 1024
RANK = 48
RHS = 8
ITERS = 2
LEAVES = 32
ROWB = 8
NPTS = 262144
N_LEAF = 32
N_ROWS = 8


def draw_tree_order(key, part):
    blocks = NPTS // PTS
    upper_bound = (1 << 30) // PTS
    scores = jax.random.randint(jax.random.fold_in(key, 11), (blocks, PTS), 0, upper_bound, dtype=jnp.int32)
    scores = scores * PTS + jnp.arange(PTS, dtype=jnp.int32)[None, :]
    within = jnp.argsort(scores, axis=1).astype(jnp.int32)
    starts = (jnp.arange(blocks, dtype=jnp.int32) * PTS)[:, None]
    return (within + starts).reshape(NPTS).astype(jnp.int32)


def steps_of(own_key, dims, pieces, smallest, largest):
    gain, own = 1.0, jax.random.fold_in(own_key, 6)
    for dim, parts in pieces:
        draws = jnp.exp(jax.random.uniform(jax.random.fold_in(own, dim), (parts,), jnp.float32, smallest / len(pieces), largest / len(pieces)))
        gain = gain * jnp.repeat(draws, dims[dim] // parts).reshape([-1 if axis == dim else 1 for axis in range(len(dims))])
    return gain


def scatter_about(own_key, dims, scale, most, cuts=(), kind=jnp.bfloat16):
    gain = steps_of(own_key, dims, cuts, -0.22, 0.18) if cuts else 1.0
    result = jax.random.normal(own_key, dims, jnp.float32) * scale * gain
    return jnp.minimum(jnp.maximum(result, -most), most).astype(kind)


def setup_inputs(seed: int = 0) -> dict:
    seeds = jax.random.split(jax.random.key(seed), 9)
    right_side = scatter_about(seeds[0], (RHS, NPTS), 1.0, 6.0, ((1, 256),), jnp.float32)
    diagonal = jnp.clip(jnp.exp(math.log(4.0) - 2.0794415 * jax.random.uniform(seeds[1], (NPTS,), jnp.float32) ** steps_of(seeds[1], (NPTS,), ((0, 256),), -0.2, 0.2)), 0.5, 4.0)
    tree_order = draw_tree_order(jax.random.fold_in(seeds[8], 71), 0)
    mid_perm = jax.random.permutation(seeds[3], LEAVES).astype(jnp.int32)
    col_factor = scatter_about(seeds[4], (NPTS, LEAVES * RANK), PTS ** -0.5, 0.1875, ((0, 256),))
    mid_factor = scatter_about(seeds[5], (LEAVES * LEAVES * RANK, ROWB * ROWB * RANK), (LEAVES * ROWB * RANK) ** -0.5, 0.0546875, ((0, 32), (1, 8)))
    pre_factor = scatter_about(seeds[6], (LEAVES * LEAVES * RANK, ROWB * ROWB * RANK), (LEAVES * ROWB * RANK) ** -0.5, 0.0546875, ((0, 32), (1, 8)))
    row_factor = scatter_about(seeds[7], (RANK, NPTS), RANK ** -0.5, 0.875, ((1, 256),))
    return {"right_side": right_side, "diagonal": diagonal, "tree_order": tree_order, "mid_perm": mid_perm, "col_factor": col_factor, "mid_factor": mid_factor, "pre_factor": pre_factor, "row_factor": row_factor}


def gram_apply(field, tree_order, mid_perm, col_factor, mid_weight, row_factor):
    leaves = N_LEAF
    row_count = N_ROWS
    blocks = leaves * row_count
    sides = field.shape[0]
    taken = jnp.take(field, tree_order, axis=1).astype(jnp.bfloat16)
    taken = taken.reshape(sides, blocks, PTS).transpose(1, 0, 2)
    col_blocks = col_factor.reshape(blocks, PTS, leaves * RANK)

    def forward_map(inputs):
        block_field, block_factor = inputs
        return jnp.dot(block_field, block_factor, preferred_element_type=jnp.float32).astype(jnp.bfloat16)

    coeffs = lax.map(forward_map, (taken, col_blocks)).reshape(blocks, sides, leaves, RANK)
    outgoing = coeffs[:, :, mid_perm, :]
    outgoing = outgoing.reshape(leaves, row_count, sides, leaves, RANK).transpose(3, 0, 1, 2, 4)
    mid_blocks = mid_weight.reshape(leaves, leaves, RANK, row_count, row_count * RANK)

    def middle_map(inputs):
        group_coef, group_weight = inputs
        return jnp.einsum('lrsk,lkrm->sm', group_coef.astype(jnp.float32), group_weight.astype(jnp.float32),
                          precision=lax.Precision.HIGHEST)

    head_coef = lax.map(middle_map, (outgoing, mid_blocks))
    head_coef = head_coef.reshape(leaves, sides, row_count, RANK).transpose(0, 2, 1, 3)
    head_coef = head_coef.reshape(blocks, sides, RANK).astype(jnp.bfloat16)
    row_blocks = row_factor.astype(jnp.float32).reshape(RANK, blocks, PTS).transpose(1, 0, 2)
    image_tree = jnp.einsum('bsk,bkn->bsn', head_coef.astype(jnp.float32), row_blocks,
                            precision=lax.Precision.HIGHEST)
    backward = jnp.einsum('bsn,bkn->bsk', image_tree, row_blocks,
                          precision=lax.Precision.HIGHEST).astype(jnp.bfloat16)
    backward = backward.reshape(leaves, row_count, sides, RANK).transpose(0, 2, 1, 3)
    backward = backward.reshape(leaves, sides, row_count * RANK)

    def middle_back(inputs):
        group_back, group_weight = inputs
        return jnp.einsum('sm,lkrm->rlsk', group_back.astype(jnp.float32), group_weight.astype(jnp.float32),
                          precision=lax.Precision.HIGHEST).astype(jnp.bfloat16)

    returned = lax.map(middle_back, (backward, mid_blocks))
    returned = returned.transpose(2, 1, 0, 3, 4).reshape(blocks, leaves, sides, RANK)
    unsent = jnp.zeros_like(returned).at[:, mid_perm].set(returned)

    def backward_map(inputs):
        block_coef, block_factor = inputs
        flattened = block_coef.transpose(1, 0, 2).reshape(sides, leaves * RANK)
        return jnp.dot(flattened, block_factor.T, preferred_element_type=jnp.float32)

    gram_tree = lax.map(backward_map, (unsent, col_blocks))
    gram_tree = gram_tree.transpose(1, 0, 2).reshape(sides, blocks * PTS)
    return jnp.zeros_like(gram_tree).at[:, tree_order].set(gram_tree)


def reference(right_side, diagonal, tree_order, mid_perm, col_factor, mid_factor, pre_factor, row_factor):
    def apply_system(field):
        return diagonal[None, :] * field + gram_apply(field, tree_order, mid_perm, col_factor, mid_factor, row_factor)

    def apply_precond(field):
        return field / diagonal[None, :] + gram_apply(field, tree_order, mid_perm, col_factor, pre_factor, row_factor)

    solution = jnp.zeros_like(right_side)
    residual = right_side
    precond = apply_precond(residual)
    direction = precond
    precond_dot = jnp.sum(residual * precond, axis=1)
    for iteration in range(ITERS):
        image = apply_system(direction)
        alpha_step = precond_dot / jnp.sum(direction * image, axis=1)
        solution = solution + alpha_step[:, None] * direction
        residual = residual - alpha_step[:, None] * image
        if iteration + 1 < ITERS:
            precond = apply_precond(residual)
            dot_next = jnp.sum(residual * precond, axis=1)
            direction = precond + (dot_next / precond_dot)[:, None] * direction
            precond_dot = dot_next
    return solution, residual
```

```python
import jax
import jax.numpy as jnp
from jax import lax
from jax.experimental import pallas as pl
from jax.experimental.pallas import tpu as pltpu
from jax.sharding import PartitionSpec as P

F32, BF16 = jnp.float32, jnp.bfloat16
MESH = pl.DeviceIdType.MESH
SIDES, PTS, RANK, LEAVES, ROWB = 8, 1024, 48, 32, 8
Z, X = 8, 4
GROUP = ROWB * RANK
LANES = 128
APPLIES = 4


def ring_distance(step, size):
    return min(step, size - step)


LEAF_STEPS = sorted(
    ((dz, dx) for dz in range(Z) for dx in range(X) if dz or dx),
    key=lambda s: -(ring_distance(s[0], Z) + ring_distance(s[1], X)),
)
ROW_STEPS = sorted(range(1, ROWB), key=lambda s: -ring_distance(s, ROWB))


def three_parts(x):
    high = x.astype(BF16)
    rest = x - high.astype(F32)
    middle = rest.astype(BF16)
    low = (rest - middle.astype(F32)).astype(BF16)
    return high, middle, low


def nt_dot(a, b):
    return lax.dot_general(a, b, (((1,), (1,)), ((), ())), preferred_element_type=F32)


def kernel(
    rs_hbm, diag_hbm, order_hbm, perm_hbm, col_hbm, mid_hbm, pre_hbm, row_hbm,
    sol_ref, res_ref,
    rs, diag, order, perm, inv_vec, inv, col, weight, row_factor, onehot,
    field, scale, slots, heads, own_gram, gram_in, gram_high, gram_low, pieces, dots_out, dots_in,
    a_out, a_in, b_out, b_in, c_out, c_in,
    local_sem, gram_sems, dots_sems, a_sems, b_sems, c_sems,
):
    leaf, row = lax.axis_index("leaf"), lax.axis_index("rows")
    z, x = leaf // X, leaf % X
    loads = []
    for i, (src, dst) in enumerate((
        (order_hbm, order), (rs_hbm, rs), (diag_hbm, diag), (perm_hbm, perm), (col_hbm, col),
        (row_hbm, row_factor), (pre_hbm, weight.at[0]), (mid_hbm, weight.at[1]),
    )):
        load = pltpu.make_async_copy(src, dst, local_sem.at[i])
        load.start()
        loads.append(load)
    l_order, l_rs, l_diag, l_perm, l_col, l_row, l_pre, l_mid = loads

    leaf_peers = [lax.rem(z + dz, Z) * X + lax.rem(x + dx, X) for dz, dx in LEAF_STEPS]
    row_peers = [lax.rem(row + d, ROWB) for d in ROW_STEPS]
    barrier = pltpu.get_barrier_semaphore()
    for q in leaf_peers:
        pl.semaphore_signal(barrier, inc=1, device_id={"leaf": q}, device_id_type=MESH)
    for r in row_peers:
        pl.semaphore_signal(barrier, inc=1, device_id={"rows": r}, device_id_type=MESH)

    lane = lax.broadcasted_iota(jnp.int32, (SIDES, LANES), 1)

    l_order.wait()
    local_index = order[...] % PTS
    step = 128
    for start in range(0, PTS, step):
        point = lax.broadcasted_iota(jnp.int32, (step, PTS), 0) + start
        onehot[pl.ds(start, step), :] = jnp.where(point == local_index, 1.0, 0.0).astype(BF16)

    l_rs.wait()
    l_diag.wait()
    stacked = jnp.concatenate([rs[...], jnp.broadcast_to(diag[...], (SIDES, PTS))], axis=0)
    parts = three_parts(stacked)
    in_tree = [jnp.dot(part, onehot[...], preferred_element_type=F32) for part in parts]
    in_tree = (in_tree[0] + in_tree[1]) + in_tree[2]
    field[0] = in_tree[:SIDES]
    scale[0] = 1.0 / in_tree[SIDES:]
    scale[1] = in_tree[SIDES:]

    def split_slots(values):
        for g in range(LEAVES):
            tile, offset = divmod(g * RANK, LANES)
            piece = values[:, tile * LANES : (tile + 1) * LANES]
            if offset + RANK > LANES:
                piece = jnp.where(lane >= offset, piece, values[:, (tile + 1) * LANES : (tile + 2) * LANES])
            if offset:
                piece = pltpu.roll(piece, LANES - offset, 1)
            slots[g] = piece

    def coefficients(apply):
        values = jnp.dot(field[apply].astype(BF16), col[...], preferred_element_type=F32)
        split_slots(values)

    l_col.wait()
    coefficients(0)

    l_row.wait()
    gram = nt_dot(row_factor[...], row_factor[...])
    own_gram[...] = jnp.concatenate([gram, jnp.zeros((RANK, LANES - RANK), F32)], axis=1)
    pieces[...] = jnp.zeros((SIDES, LANES), F32)

    l_perm.wait()
    inverse = jnp.zeros((SIDES, LANES), jnp.int32)
    for q in range(LEAVES):
        inverse = jnp.where(lane == perm[q], q, inverse)
    inv_vec[...] = inverse
    inv_copy = pltpu.make_async_copy(inv_vec, inv, local_sem.at[8])
    inv_copy.start()
    l_pre.wait()
    l_mid.wait()
    inv_copy.wait()

    pl.semaphore_wait(barrier, len(LEAF_STEPS) + len(ROW_STEPS))

    gram_copies = [
        pltpu.make_async_remote_copy(
            src_ref=own_gram, dst_ref=gram_in.at[row], send_sem=gram_sems.at[0], recv_sem=gram_sems.at[1],
            device_id={"rows": r}, device_id_type=MESH,
        )
        for r in row_peers
    ]

    def send_slots(apply, out, into, sems, slot_of, extra):
        for i, q in enumerate(leaf_peers):
            value = jnp.where(lane < RANK, slots[slot_of(q)], extra)
            out[apply, i] = value.astype(BF16)
            pltpu.make_async_remote_copy(
                src_ref=out.at[apply, i], dst_ref=into.at[apply, leaf],
                send_sem=sems.at[0, apply], recv_sem=sems.at[1, apply],
                device_id={"leaf": q}, device_id_type=MESH,
            ).start()
        into[apply, leaf] = jnp.where(lane < RANK, slots[slot_of(leaf)], extra).astype(BF16)

    def leaf_wait(apply, out, into, sems):
        return pltpu.make_async_remote_copy(
            src_ref=out.at[apply], dst_ref=into.at[apply, pl.ds(0, LEAVES - 1)],
            send_sem=sems.at[0, apply], recv_sem=sems.at[1, apply],
            device_id={"leaf": leaf_peers[0]}, device_id_type=MESH,
        )

    def joined(apply, into, place_of):
        tiles = [None] * (LEAVES * RANK // LANES)

        def put(tile, value):
            tiles[tile] = value if tiles[tile] is None else tiles[tile] + value

        for s in range(LEAVES):
            tile, offset = divmod(s * RANK, LANES)
            value = into[apply, place_of(s)].astype(F32)
            value = jnp.where(lane < RANK, value, 0.0)
            if offset:
                value = pltpu.roll(value, offset, 1)
            if offset + RANK > LANES:
                put(tile, jnp.where(lane >= offset, value, 0.0))
                put(tile + 1, jnp.where(lane < offset, value, 0.0))
            else:
                put(tile, value)
        return jnp.concatenate(tiles, axis=1).astype(BF16)

    zero = jnp.zeros((SIDES, LANES), F32)

    def one_apply(apply, carry):
        kind = apply % 2
        send_slots(apply, a_out, a_in, a_sems, lambda q: perm[q], zero)

        @pl.when(apply == 0)
        def _():
            for copy in gram_copies:
                copy.start()
            gram_in[row] = own_gram[...]
            pltpu.make_async_remote_copy(
                src_ref=gram_in.at[pl.ds(0, ROWB - 1)], dst_ref=gram_in.at[pl.ds(0, ROWB - 1)],
                send_sem=gram_sems.at[0], recv_sem=gram_sems.at[1],
                device_id={"rows": row_peers[0]}, device_id_type=MESH,
            ).wait_recv()
            wide = lax.broadcasted_iota(jnp.int32, (RANK, LANES), 1)
            for j in range(ROWB):
                tile, offset = divmod(j * RANK, LANES)
                value = gram_in[j]
                if offset:
                    value = pltpu.roll(value, offset, 1)
                parts = [jnp.zeros((RANK, LANES), F32)] * (GROUP // LANES)
                if offset + RANK > LANES:
                    parts[tile] = jnp.where(wide >= offset, value, 0.0)
                    parts[tile + 1] = jnp.where(wide < offset, value, 0.0)
                else:
                    parts[tile] = value
                whole = jnp.concatenate(parts, axis=1)
                high = whole.astype(BF16)
                gram_high[pl.ds(j * RANK, RANK), :] = high
                gram_low[pl.ds(j * RANK, RANK), :] = (whole - high.astype(F32)).astype(BF16)

        @pl.when(apply == APPLIES - 1)
        def _():
            r0, z0, w0, y = field[0], field[1], field[2], field[3]
            d = scale[1]
            sums = [r0 * z0, z0 * w0, r0 * y, w0 * y, d * z0 * y, d * y * y]
            out = zero
            for i, products in enumerate(sums):
                out = jnp.where(lane == i, jnp.sum(products, axis=1, keepdims=True), out)
            dots_out[...] = out
            for r in row_peers:
                pltpu.make_async_remote_copy(
                    src_ref=dots_out, dst_ref=dots_in.at[row], send_sem=dots_sems.at[0], recv_sem=dots_sems.at[1],
                    device_id={"rows": r}, device_id_type=MESH,
                ).start()
            dots_in[row] = out

        leaf_wait(apply, a_out, a_in, a_sems).wait_recv()
        incoming = joined(apply, a_in, lambda s: s)
        partial = jnp.dot(incoming, weight[kind], preferred_element_type=F32)
        b_out[apply] = partial
        for r in row_peers:
            pltpu.make_async_remote_copy(
                src_ref=b_out.at[apply], dst_ref=b_in.at[apply, row],
                send_sem=b_sems.at[0, apply], recv_sem=b_sems.at[1, apply],
                device_id={"rows": r}, device_id_type=MESH,
            ).start()
        b_in[apply, row] = partial
        pltpu.make_async_remote_copy(
            src_ref=b_in.at[apply, pl.ds(0, ROWB - 1)], dst_ref=b_in.at[apply, pl.ds(0, ROWB - 1)],
            send_sem=b_sems.at[0, apply], recv_sem=b_sems.at[1, apply],
            device_id={"rows": row_peers[0]}, device_id_type=MESH,
        ).wait_recv()
        total = b_in[apply, 0]
        for r in range(1, ROWB):
            total = total + b_in[apply, r]
        head = total.astype(BF16)
        heads[apply] = head.astype(F32)
        back = jnp.dot(head, gram_high[...], preferred_element_type=F32)
        back = back + jnp.dot(head, gram_low[...], preferred_element_type=F32)

        @pl.when(apply == APPLIES - 1)
        def _():
            pltpu.make_async_remote_copy(
                src_ref=dots_in.at[pl.ds(0, ROWB - 1)], dst_ref=dots_in.at[pl.ds(0, ROWB - 1)],
                send_sem=dots_sems.at[0], recv_sem=dots_sems.at[1],
                device_id={"rows": row_peers[0]}, device_id_type=MESH,
            ).wait_recv()
            dots = dots_in[0]
            for r in range(1, ROWB):
                dots = dots + dots_in[r]
            dots = jnp.where(lane == 6, jnp.sum(heads[1] * back, axis=1, keepdims=True), dots)
            dots = jnp.where(lane == 7, jnp.sum(heads[3] * back, axis=1, keepdims=True), dots)
            high, middle, low = three_parts(dots)
            pieces[...] = (
                pltpu.roll(high.astype(F32), 64, 1)
                + pltpu.roll(middle.astype(F32), 72, 1)
                + pltpu.roll(low.astype(F32), 80, 1)
            )

        split_slots(nt_dot(back.astype(BF16), weight[kind]))
        send_slots(apply, c_out, c_in, c_sems, lambda l: l, pieces[...])
        leaf_wait(apply, c_out, c_in, c_sems).wait_recv()
        unsent = joined(apply, c_in, lambda s: inv[0, s])
        image = nt_dot(unsent, col[...])
        field[apply + 1] = scale[kind] * field[apply] + image

        @pl.when(apply < APPLIES - 1)
        def _():
            coefficients(apply + 1)

        return carry

    lax.fori_loop(0, APPLIES, one_apply, 0)

    total = c_in[APPLIES - 1, 0].astype(F32)
    for q in range(1, LEAVES):
        total = total + c_in[APPLIES - 1, q].astype(F32)

    def dot_value(i):
        return total[:, 64 + i : 65 + i] + total[:, 72 + i : 73 + i] + total[:, 80 + i : 81 + i]

    rz, zw, ry, wy = (dot_value(i) for i in range(4))
    zt, yt = dot_value(4) + dot_value(6), dot_value(5) + dot_value(7)
    alpha = rz / zw
    rz_next = (rz - alpha * zw) - alpha * (ry - alpha * wy)
    along = 1.0 + rz_next / rz
    alpha_next = rz_next / (along * along * zw - along * alpha * (zt + wy) + alpha * alpha * yt)
    r0, z0, w0, y, t = (field[i] for i in range(5))
    solution_tree = alpha * z0 + alpha_next * (along * z0 - alpha * y)
    residual_tree = (r0 - alpha * w0) - alpha_next * (along * w0 - alpha * t)
    parts = three_parts(jnp.concatenate([solution_tree, residual_tree], axis=0))
    back_parts = [nt_dot(part, onehot[...]) for part in parts]
    result = (back_parts[0] + back_parts[1]) + back_parts[2]
    sol_ref[...] = result[:SIDES]
    res_ref[...] = result[SIDES:]

    for copy in gram_copies:
        copy.wait_send()
    for apply in range(APPLIES):
        leaf_wait(apply, a_out, a_in, a_sems).wait_send()
        leaf_wait(apply, c_out, c_in, c_sems).wait_send()
        for r in row_peers:
            pltpu.make_async_remote_copy(
                src_ref=b_out.at[apply], dst_ref=b_in.at[apply, row],
                send_sem=b_sems.at[0, apply], recv_sem=b_sems.at[1, apply],
                device_id={"rows": r}, device_id_type=MESH,
            ).wait_send()
    for r in row_peers:
        pltpu.make_async_remote_copy(
            src_ref=dots_out, dst_ref=dots_in.at[row], send_sem=dots_sems.at[0], recv_sem=dots_sems.at[1],
            device_id={"rows": r}, device_id_type=MESH,
        ).wait_send()


def per_device(
    right_side, diagonal, tree_order, mid_perm, col_factor, mid_factor, pre_factor, row_factor
):
    any_space = pl.BlockSpec(memory_space=pl.ANY)
    vmem = pl.BlockSpec(memory_space=pltpu.VMEM)
    return pl.pallas_call(
        kernel,
        out_shape=(jax.ShapeDtypeStruct((SIDES, PTS), F32),) * 2,
        in_specs=[any_space] * 8,
        out_specs=(vmem, vmem),
        scratch_shapes=[
            pltpu.VMEM((SIDES, PTS), F32),
            pltpu.VMEM((1, PTS), F32),
            pltpu.VMEM((1, PTS), jnp.int32),
            pltpu.SMEM((LEAVES,), jnp.int32),
            pltpu.VMEM((SIDES, LANES), jnp.int32),
            pltpu.SMEM((SIDES, LANES), jnp.int32),
            pltpu.VMEM((PTS, LEAVES * RANK), BF16),
            pltpu.VMEM((2, LEAVES * RANK, GROUP), BF16),
            pltpu.VMEM((RANK, PTS), BF16),
            pltpu.VMEM((PTS, PTS), BF16),
            pltpu.VMEM((APPLIES + 1, SIDES, PTS), F32),
            pltpu.VMEM((2, SIDES, PTS), F32),
            pltpu.VMEM((LEAVES, SIDES, LANES), F32),
            pltpu.VMEM((APPLIES, SIDES, GROUP), F32),
            pltpu.VMEM((RANK, LANES), F32),
            pltpu.VMEM((ROWB, RANK, LANES), F32),
            pltpu.VMEM((GROUP, GROUP), BF16),
            pltpu.VMEM((GROUP, GROUP), BF16),
            pltpu.VMEM((SIDES, LANES), F32),
            pltpu.VMEM((SIDES, LANES), F32),
            pltpu.VMEM((ROWB, SIDES, LANES), F32),
            pltpu.VMEM((APPLIES, LEAVES - 1, SIDES, LANES), BF16),
            pltpu.VMEM((APPLIES, LEAVES, SIDES, LANES), BF16),
            pltpu.VMEM((APPLIES, SIDES, GROUP), F32),
            pltpu.VMEM((APPLIES, ROWB, SIDES, GROUP), F32),
            pltpu.VMEM((APPLIES, LEAVES - 1, SIDES, LANES), BF16),
            pltpu.VMEM((APPLIES, LEAVES, SIDES, LANES), BF16),
            pltpu.SemaphoreType.DMA((9,)),
            pltpu.SemaphoreType.DMA((2,)),
            pltpu.SemaphoreType.DMA((2,)),
            pltpu.SemaphoreType.DMA((2, APPLIES)),
            pltpu.SemaphoreType.DMA((2, APPLIES)),
            pltpu.SemaphoreType.DMA((2, APPLIES)),
        ],
        compiler_params=pltpu.CompilerParams(
            collective_id=0, has_side_effects=True, vmem_limit_bytes=60000 * 1024
        ),
    )(
        right_side, diagonal.reshape(1, PTS), tree_order.reshape(1, PTS), mid_perm,
        col_factor, mid_factor, pre_factor, row_factor,
    )


def solution(mesh):
    every = ("leaf", "rows")
    return jax.shard_map(
        per_device,
        mesh=mesh,
        in_specs=(
            P(None, every), P(every), P(every), P(),
            P(every, None), P("leaf", "rows"), P("leaf", "rows"), P(None, every),
        ),
        out_specs=(P(None, every), P(None, every)),
        check_vma=False,
    )
```

```python
import jax
import jax.numpy as jnp
from jax import lax
from jax.experimental import pallas as pl
from jax.experimental.pallas import tpu as pltpu
from jax.sharding import PartitionSpec as P

F32, BF16 = jnp.float32, jnp.bfloat16
MESH = pl.DeviceIdType.MESH
SIDES, PTS, RANK, LEAVES, ROWB = 8, 1024, 48, 32, 8
Z, X = 8, 4
CHUNKS, EACH = 4, 8
GROUP = ROWB * RANK
LANES = 128
TILES = GROUP // LANES
APPLIES = 4


def ring_distance(step, size):
    return min(step, size - step)


LEAF_STEPS = sorted(
    ((dz, dx) for dz in range(Z) for dx in range(X) if dz or dx),
    key=lambda s: -(ring_distance(s[0], Z) + ring_distance(s[1], X)),
)
ROW_STEPS = sorted(range(1, ROWB), key=lambda s: -ring_distance(s, ROWB))


def three_parts(x):
    high = x.astype(BF16)
    rest = x - high.astype(F32)
    middle = rest.astype(BF16)
    low = (rest - middle.astype(F32)).astype(BF16)
    return high, middle, low


def nn_dot(a, b):
    return jnp.dot(a, b, preferred_element_type=F32)


def nt_dot(a, b):
    return lax.dot_general(a, b, (((1,), (1,)), ((), ())), preferred_element_type=F32)


def kernel(
    rs_hbm, diag_hbm, order_hbm, perm_hbm, col_hbm, mid_hbm, pre_hbm, row_hbm,
    x1_ref, p1_ref, r1_ref, image_ref, alpha_ref,
    rs, diag, order, perm, col, col_t, col_q, back_q, weight, returner, row_factor, onehot,
    field, scale, points, first_slots, slots, own_gram, gram_in, gram_high, gram_low, dots_out, dots_in, dots_sum,
    a_out, a_in, b_out, b_in, c_out, c_in,
    local_sem, gram_sems, dots_sems, a_send, a_recv, b_sems, c_send, c_recv,
):
    leaf, row = lax.axis_index("leaf"), lax.axis_index("rows")
    z, x = leaf // X, leaf % X
    own_chunk = z // 2
    leaf_peers = [lax.rem(z + dz, Z) * X + lax.rem(x + dx, X) for dz, dx in LEAF_STEPS]
    row_peers = [lax.rem(row + d, ROWB) for d in ROW_STEPS]
    barrier = pltpu.get_barrier_semaphore()
    for q in leaf_peers:
        pl.semaphore_signal(barrier, inc=1, device_id={"leaf": q}, device_id_type=MESH)
    for r in row_peers:
        pl.semaphore_signal(barrier, inc=1, device_id={"rows": r}, device_id_type=MESH)
    loads = []
    for i, (src, dst) in enumerate((
        (order_hbm, order), (rs_hbm, rs), (col_hbm, col), (row_hbm, row_factor), (perm_hbm, perm),
        (diag_hbm, diag), (pre_hbm, weight.at[0]), (mid_hbm, weight.at[1]),
    )):
        load = pltpu.make_async_copy(src, dst, local_sem.at[i])
        load.start()
        loads.append(load)
    l_order, l_rs, l_col, l_row, l_perm, l_diag = loads[:6]

    lane = lax.broadcasted_iota(jnp.int32, (SIDES, LANES), 1)
    zero = jnp.zeros((SIDES, LANES), F32)

    def chunk(step):
        return lax.rem(own_chunk + step, CHUNKS)

    turn = lax.rem(z, 2)
    far_z = (lax.rem(z + 4, Z), lax.rem(z + 5 - 2 * turn, Z))
    near_z = [lax.rem(z + 3 + 2 * turn, Z)] + [lax.rem(z + dz, Z) for dz in (2, 6, 1, 7, 0)]

    def by_distance(planes):
        hops = {2: 2, 1: 1, 3: 1, 0: 0}
        return [
            (zz, lax.rem(x + dx, X))
            for _, _, zz, dx in sorted(
                ((-(far + hops[dx]), i, zz, dx) for i, (far, zz) in enumerate(planes) for dx in hops if far or dx),
                key=lambda item: item[:2],
            )
        ]

    def group_of(zz):
        return lax.rem(zz // 2 - own_chunk + CHUNKS, 2)

    far_peers = by_distance(list(zip((4, 3), far_z)))
    near_peers = by_distance(list(zip((3, 2, 2, 1, 1, 0), near_z)))

    def slot_of(values, place, target):
        tile, offset = divmod(place * RANK, LANES)
        piece = values[:, tile * LANES : (tile + 1) * LANES]
        if offset + RANK > LANES:
            piece = jnp.where(lane >= offset, piece, values[:, (tile + 1) * LANES : (tile + 2) * LANES])
        shift = (target - offset) % LANES
        return pltpu.roll(piece, shift, 1) if shift else piece

    def leaf_send(apply, n, out, into, send, recv, q):
        pltpu.make_async_remote_copy(
            src_ref=out.at[apply, n], dst_ref=into.at[apply, leaf],
            send_sem=send.at[apply], recv_sem=recv, device_id={"leaf": q}, device_id_type=MESH,
        ).start()

    def put_slots(base, values, extra):
        for i in range(values.shape[1] // RANK):
            slots[base + i] = jnp.where(lane < RANK, slot_of(values, i, 0), extra)

    def send_peers(apply, start, peers, out, into, send, recv):
        for n, (zz, xx) in enumerate(peers):
            q = zz * X + xx
            out[apply, start + n] = slots[q].astype(BF16)
            leaf_send(apply, start + n, out, into, send, recv(zz), q)

    def leaf_wait(apply, count, into, send, recv):
        part = into.at[apply, pl.ds(0, count)]
        pltpu.make_async_remote_copy(
            src_ref=part, dst_ref=part, send_sem=send.at[apply], recv_sem=recv,
            device_id={"leaf": leaf_peers[0]}, device_id_type=MESH,
        ).wait_recv()

    def joined(apply, base, into):
        tiles = [None] * TILES

        def put(tile, value):
            tiles[tile] = value if tiles[tile] is None else tiles[tile] + value

        for i in range(EACH):
            tile, offset = divmod(i * RANK, LANES)
            value = jnp.where(lane < RANK, into[apply, base + i].astype(F32), 0.0)
            if offset:
                value = pltpu.roll(value, offset, 1)
            if offset + RANK > LANES:
                put(tile, jnp.where(lane >= offset, value, 0.0))
                put(tile + 1, jnp.where(lane < offset, value, 0.0))
            else:
                put(tile, value)
        return jnp.concatenate(tiles, axis=1).astype(BF16)

    def rows_copy(src, dst, sems, r):
        return pltpu.make_async_remote_copy(
            src_ref=src, dst_ref=dst, send_sem=sems.at[0], recv_sem=sems.at[1],
            device_id={"rows": r}, device_id_type=MESH,
        )

    def rows_wait(into, sems):
        part = into.at[pl.ds(0, ROWB - 1)]
        return rows_copy(part, part, sems, row_peers[0])

    def summed(into):
        total = into[0]
        for r in range(1, ROWB):
            total = total + into[r]
        return total

    def side_sum(products):
        return jnp.sum(products, axis=1, keepdims=True)

    def to_points(values):
        parts = [nt_dot(part, onehot[...]) for part in three_parts(values)]
        return (parts[0] + parts[1]) + parts[2]

    l_order.wait()
    local_index = order[...] % PTS
    step = 128
    for start in range(0, PTS, step):
        point = lax.broadcasted_iota(jnp.int32, (step, PTS), 0) + start
        onehot[pl.ds(start, step), :] = jnp.where(point == local_index, 1.0, 0.0).astype(BF16)
    l_rs.wait()
    rs_high, rs_middle, rs_low = three_parts(rs[...])
    tree_high = nn_dot(rs_high, onehot[...])
    l_col.wait()
    values = nn_dot(tree_high.astype(BF16), col[...])
    for g in range(LEAVES):
        tile, offset = divmod(g * RANK, LANES)
        piece = values[:, tile * LANES : (tile + 1) * LANES]
        if offset + RANK > LANES:
            piece = jnp.where(lane >= offset, piece, values[:, (tile + 1) * LANES : (tile + 2) * LANES])
        if offset:
            piece = pltpu.roll(piece, LANES - offset, 1)
        first_slots[g] = jnp.where(lane < RANK, piece, 0.0)
    l_perm.wait()
    l_row.wait()
    pl.semaphore_wait(barrier, len(LEAF_STEPS) + len(ROW_STEPS))
    for n, q in enumerate(leaf_peers):
        a_out[0, n] = first_slots[perm[q]].astype(BF16)
        leaf_send(0, n, a_out, a_in, a_send, a_recv.at[0], q)
    a_in[0, leaf] = first_slots[perm[leaf]].astype(BF16)

    @pl.when(leaf >= 0)
    def _():
        gram = nt_dot(row_factor[...], row_factor[...])
        own_gram[...] = jnp.concatenate([gram, jnp.zeros((RANK, LANES - RANK), F32)], axis=1)
        for r in row_peers:
            rows_copy(own_gram, gram_in.at[row], gram_sems, r).start()
        gram_in[row] = own_gram[...]

    @pl.when(leaf >= 0)
    def _():
        tree_middle = nn_dot(jnp.concatenate([rs_middle, rs_low], axis=0), onehot[...])
        field[0] = (tree_high + tree_middle[:SIDES]) + tree_middle[SIDES:]
        for t in range(LEAVES * RANK // LANES):
            turned = col[:, t * LANES : (t + 1) * LANES].T
            start = 0
            while start < LANES:
                g, first = divmod(t * LANES + start, RANK)
                count = min(RANK - first, LANES - start)
                col_t[g, pl.ds(first, count), :] = turned[start : start + count]
                start += count
        for q in range(LEAVES):
            c, i = divmod(q, EACH)
            back_q[0, c, pl.ds(i * RANK, RANK), :] = col_t[perm[q]]
        l_diag.wait()
        diag_points = jnp.broadcast_to(diag[...], (SIDES, PTS))
        diag_tree = [nn_dot(part, onehot[...]) for part in three_parts(diag_points)]
        diag_tree = (diag_tree[0] + diag_tree[1]) + diag_tree[2]
        scale[0] = 1.0 / diag_tree
        scale[1] = diag_tree
        for load in loads[6:]:
            load.wait()


    def build_gram():
        rows_wait(gram_in, gram_sems).wait_recv()
        wide = lax.broadcasted_iota(jnp.int32, (RANK, LANES), 1)
        for j in range(ROWB):
            tile, offset = divmod(j * RANK, LANES)
            value = gram_in[j]
            if offset:
                value = pltpu.roll(value, offset, 1)
            parts = [jnp.zeros((RANK, LANES), F32)] * TILES
            if offset + RANK > LANES:
                parts[tile] = jnp.where(wide >= offset, value, 0.0)
                parts[tile + 1] = jnp.where(wide < offset, value, 0.0)
            else:
                parts[tile] = value
            whole = jnp.concatenate(parts, axis=1)
            high = whole.astype(BF16)
            gram_high[pl.ds(j * RANK, RANK), :] = high
            gram_low[pl.ds(j * RANK, RANK), :] = (whole - high.astype(F32)).astype(BF16)

    def build_returner(kind):
        for c in range(CHUNKS):
            rows = pl.ds(c * GROUP, GROUP)
            product = nt_dot(gram_high[...], weight[kind, rows]) + nt_dot(gram_low[...], weight[kind, rows])
            returner[kind, :, c * GROUP : (c + 1) * GROUP] = product.astype(BF16)

    def build_last(chunks):
        for c in chunks:
            back_q[1, c] = nt_dot(back_q[0, c], onehot[...]).astype(BF16)

    earlier_head = None
    dots_total = None
    for apply in range(APPLIES):
        kind, last = apply % 2, apply == APPLIES - 1
        @pl.when(leaf >= 0)
        def _():
            if 0 < apply:
                points[apply] = to_points(field[apply])
            if last:
                r0, z0, w0, y, d = field[0], field[1], field[2], field[3], scale[1]
                out = zero
                for i, products in enumerate([r0 * z0, z0 * w0, r0 * y, w0 * y, d * z0 * y, d * y * y]):
                    out = jnp.where(lane == i, side_sum(products), out)
                dots_out[...] = out
                for r in row_peers:
                    rows_copy(dots_out, dots_in.at[row], dots_sems, r).start()
                dots_in[row] = out

        leaf_wait(apply, LEAVES - 1, a_in, a_send, a_recv.at[apply])
        incoming = jnp.concatenate([joined(apply, c * EACH, a_in) for c in range(CHUNKS)], axis=1)
        partial = nn_dot(incoming, weight[kind])
        b_out[apply] = partial
        for r in row_peers:
            rows_copy(b_out.at[apply], b_in.at[apply, row], b_sems.at[apply], r).start()
        b_in[apply, row] = partial
        @pl.when(leaf >= 0)
        def _():
            if apply == 0:
                build_gram()
                build_returner(0)
            if last:
                rows_wait(dots_in, dots_sems).wait_recv()
                dots_sum[...] = summed(dots_in)

        rows_wait(b_in.at[apply], b_sems.at[apply]).wait_recv()
        head = summed(b_in.at[apply]).astype(BF16)
        extra = zero
        if apply == 1:
            earlier_head = head.astype(F32)
        if last:
            back = nn_dot(head, gram_high[...]) + nn_dot(head, gram_low[...])
            dots = jnp.where(lane == 6, side_sum(earlier_head * back), dots_sum[...])
            dots = jnp.where(lane == 7, side_sum(head.astype(F32) * back), dots)
            high, middle, low = three_parts(dots)
            extra = (
                pltpu.roll(high.astype(F32), 64, 1)
                + pltpu.roll(middle.astype(F32), 72, 1)
                + pltpu.roll(low.astype(F32), 80, 1)
            )
        put_slots(0, nn_dot(head, returner[kind]), extra)
        send_peers(apply, 0, far_peers, c_out, c_in, c_send, lambda zz: c_recv.at[apply, 2])
        send_peers(apply, EACH, near_peers, c_out, c_in, c_send, lambda zz: c_recv.at[apply, group_of(zz)])
        c_in[apply, leaf] = slots[leaf].astype(BF16)
        @pl.when(leaf >= 0)
        def _():
            if apply == 0:
                for c in range(CHUNKS):
                    col_q[c] = back_q[0, c].T
                build_returner(1)
            if apply in (1, 2):
                build_last((0, 1) if apply == 1 else (2, 3))

        image = None
        for group, (steps, count) in enumerate((((0,), EACH - 1), ((1, 3), 2 * EACH), ((2,), EACH))):
            leaf_wait(apply, count, c_in, c_send, c_recv.at[apply, group])
            for step in steps:
                c = chunk(step)
                product = nn_dot(joined(apply, c * EACH, c_in), back_q[1 if last else 0, c])
                image = product if image is None else image + product
                if last:
                    for i in range(EACH):
                        value = c_in[apply, c * EACH + i].astype(F32)
                        dots_total = value if dots_total is None else dots_total + value
        if not last:
            following = scale[kind] * field[apply] + image
            field[apply + 1] = following
            taken = following.astype(BF16)
            c = chunk(2)
            put_slots(c * EACH, nn_dot(taken, col_q[c]), zero)
            send_peers(apply + 1, 0, far_peers, a_out, a_in, a_send, lambda zz: a_recv.at[apply + 1])
            others = [(chunk(step), nn_dot(taken, col_q[chunk(step)])) for step in (1, 3, 0)]
            for c, values in others:
                put_slots(c * EACH, values, zero)
            send_peers(apply + 1, EACH, near_peers, a_out, a_in, a_send, lambda zz: a_recv.at[apply + 1])
            a_in[apply + 1, leaf] = slots[leaf].astype(BF16)

    def dot_value(i):
        return (
            dots_total[:, 64 + i : 65 + i] + dots_total[:, 72 + i : 73 + i] + dots_total[:, 80 + i : 81 + i]
        )

    rz, zw, ry, wy = (dot_value(i) for i in range(4))
    zt, yt = dot_value(4) + dot_value(6), dot_value(5) + dot_value(7)
    alpha = rz / zw
    rz_next = (rz - alpha * zw) - alpha * (ry - alpha * wy)
    along = 1.0 + rz_next / rz
    alpha_next = rz_next / (along * along * zw - along * alpha * (zt + wy) + alpha * alpha * yt)
    z0, w0, y = points[1], points[2], points[3]
    t = diag[...] * y + image
    x1_ref[...] = alpha * z0
    p1_ref[...] = along * z0 - alpha * y
    r1_ref[...] = rs[...] - alpha * w0
    image_ref[...] = along * w0 - alpha * t
    alpha_ref[...] = jnp.broadcast_to(alpha_next, (SIDES, PTS))

    for r in row_peers:
        rows_copy(own_gram, gram_in.at[row], gram_sems, r).wait_send()
        rows_copy(dots_out, dots_in.at[row], dots_sems, r).wait_send()
    for apply in range(APPLIES):
        for out, send in ((a_out, a_send), (c_out, c_send)):
            pltpu.make_async_remote_copy(
                src_ref=out.at[apply], dst_ref=out.at[apply],
                send_sem=send.at[apply], recv_sem=a_recv.at[apply],
                device_id={"leaf": leaf_peers[0]}, device_id_type=MESH,
            ).wait_send()
        for r in row_peers:
            rows_copy(b_out.at[apply], b_in.at[apply, row], b_sems.at[apply], r).wait_send()


def per_device(
    right_side, diagonal, tree_order, mid_perm, col_factor, mid_factor, pre_factor, row_factor
):
    hbm = pl.BlockSpec(memory_space=pl.ANY)
    vmem = pl.BlockSpec(memory_space=pltpu.VMEM)
    diagonal, tree_order = diagonal.reshape(1, PTS), tree_order.reshape(1, PTS)
    right_side, diagonal, tree_order, mid_perm, col_factor, mid_factor, pre_factor, row_factor = (
        pltpu.with_memory_space_constraint(array, pltpu.HBM)
        for array in (right_side, diagonal, tree_order, mid_perm, col_factor, mid_factor, pre_factor, row_factor)
    )
    x1, p1, r1, image, alpha = pl.pallas_call(
        kernel,
        out_shape=(jax.ShapeDtypeStruct((SIDES, PTS), F32),) * 5,
        in_specs=[hbm] * 8,
        out_specs=(vmem,) * 5,
        scratch_shapes=[
            pltpu.VMEM((SIDES, PTS), F32),
            pltpu.VMEM((1, PTS), F32),
            pltpu.VMEM((1, PTS), jnp.int32),
            pltpu.SMEM((LEAVES,), jnp.int32),
            pltpu.VMEM((PTS, LEAVES * RANK), BF16),
            pltpu.VMEM((LEAVES, RANK, PTS), BF16),
            pltpu.VMEM((CHUNKS, PTS, GROUP), BF16),
            pltpu.VMEM((2, CHUNKS, GROUP, PTS), BF16),
            pltpu.VMEM((2, LEAVES * RANK, GROUP), BF16),
            pltpu.VMEM((2, GROUP, LEAVES * RANK), BF16),
            pltpu.VMEM((RANK, PTS), BF16),
            pltpu.VMEM((PTS, PTS), BF16),
            pltpu.VMEM((APPLIES, SIDES, PTS), F32),
            pltpu.VMEM((2, SIDES, PTS), F32),
            pltpu.VMEM((APPLIES, SIDES, PTS), F32),
            pltpu.VMEM((LEAVES, SIDES, LANES), F32),
            pltpu.VMEM((LEAVES, SIDES, LANES), F32),
            pltpu.VMEM((RANK, LANES), F32),
            pltpu.VMEM((ROWB, RANK, LANES), F32),
            pltpu.VMEM((GROUP, GROUP), BF16),
            pltpu.VMEM((GROUP, GROUP), BF16),
            pltpu.VMEM((SIDES, LANES), F32),
            pltpu.VMEM((ROWB, SIDES, LANES), F32),
            pltpu.VMEM((SIDES, LANES), F32),
            pltpu.VMEM((APPLIES, LEAVES - 1, SIDES, LANES), BF16),
            pltpu.VMEM((APPLIES, LEAVES, SIDES, LANES), BF16),
            pltpu.VMEM((APPLIES, SIDES, GROUP), F32),
            pltpu.VMEM((APPLIES, ROWB, SIDES, GROUP), F32),
            pltpu.VMEM((APPLIES, LEAVES - 1, SIDES, LANES), BF16),
            pltpu.VMEM((APPLIES, LEAVES, SIDES, LANES), BF16),
            pltpu.SemaphoreType.DMA((8,)),
            pltpu.SemaphoreType.DMA((2,)),
            pltpu.SemaphoreType.DMA((2,)),
            pltpu.SemaphoreType.DMA((APPLIES,)),
            pltpu.SemaphoreType.DMA((APPLIES,)),
            pltpu.SemaphoreType.DMA((APPLIES, 2)),
            pltpu.SemaphoreType.DMA((APPLIES,)),
            pltpu.SemaphoreType.DMA((APPLIES, 3)),
        ],
        compiler_params=pltpu.CompilerParams(
            collective_id=0, has_side_effects=True, vmem_limit_bytes=40000 * 1024
        ),
    )(
        right_side, diagonal, tree_order, mid_perm,
        col_factor, mid_factor, pre_factor, row_factor,
    )
    return x1 + alpha * p1, r1 - alpha * image


def solution(mesh):
    every = ("leaf", "rows")
    return jax.shard_map(
        per_device,
        mesh=mesh,
        in_specs=(
            P(None, every), P(every), P(every), P(),
            P(every, None), P("leaf", "rows"), P("leaf", "rows"), P(None, every),
        ),
        out_specs=(P(None, every), P(None, every)),
        check_vma=False,
    )
```

```python
import jax
import jax.numpy as jnp
from jax import lax
from jax.experimental import pallas as pl
from jax.experimental.pallas import tpu as pltpu
from jax.sharding import PartitionSpec as P

F32, BF16 = jnp.float32, jnp.bfloat16
MESH = pl.DeviceIdType.MESH
SIDES, PTS, RANK, LEAVES, ROWB = 8, 1024, 48, 32, 8
Z, X = 8, 4
PLANE = X * RANK
FAR_TURNS, NEAR_TURNS = (4, 3, 5), (0, 1, 7, 2, 6)
GROUP = ROWB * RANK
LANES = 128
TILES = GROUP // LANES
FAR_COUNT, NEAR_COUNT = 3 * X, 5 * X - 1
APPLIES = 4


def ring_distance(step, size):
    return min(step, size - step)


LEAF_STEPS = sorted(
    ((dz, dx) for dz in range(Z) for dx in range(X) if dz or dx),
    key=lambda s: -(ring_distance(s[0], Z) + ring_distance(s[1], X)),
)
ROW_STEPS = sorted(range(1, ROWB), key=lambda s: -ring_distance(s, ROWB))


def three_parts(x):
    high = x.astype(BF16)
    rest = x - high.astype(F32)
    middle = rest.astype(BF16)
    low = (rest - middle.astype(F32)).astype(BF16)
    return high, middle, low


def nn_dot(a, b):
    return jnp.dot(a, b, preferred_element_type=F32)


def nt_dot(a, b):
    return lax.dot_general(a, b, (((1,), (1,)), ((), ())), preferred_element_type=F32)


def kernel(
    rs_hbm, diag_hbm, order_hbm, perm_hbm, col_hbm, mid_hbm, pre_hbm, row_hbm,
    x1_ref, p1_ref, r1_ref, image_ref, alpha_ref,
    rs, diag, order, perm, col, col_t, col_q, back_q, weight, returner, row_factor, onehot,
    field, scale, points, first_slots, slots, own_gram, gram_in, gram_high, gram_low, dots_out, dots_in, dots_sum,
    a_out, a_in, b_out, b_in, c_out, c_in,
    local_sem, gram_sems, dots_sems, a_send, a_recv, b_sems, c_send, c_recv,
):
    leaf, row = lax.axis_index("leaf"), lax.axis_index("rows")
    z, x = leaf // X, leaf % X
    leaf_peers = [lax.rem(z + dz, Z) * X + lax.rem(x + dx, X) for dz, dx in LEAF_STEPS]
    row_peers = [lax.rem(row + d, ROWB) for d in ROW_STEPS]
    barrier = pltpu.get_barrier_semaphore()
    for q in leaf_peers:
        pl.semaphore_signal(barrier, inc=1, device_id={"leaf": q}, device_id_type=MESH)
    for r in row_peers:
        pl.semaphore_signal(barrier, inc=1, device_id={"rows": r}, device_id_type=MESH)
    loads = []
    for i, (src, dst) in enumerate((
        (order_hbm, order), (rs_hbm, rs), (col_hbm, col), (row_hbm, row_factor), (perm_hbm, perm),
        (diag_hbm, diag), (pre_hbm, weight.at[0]), (mid_hbm, weight.at[1]),
    )):
        load = pltpu.make_async_copy(src, dst, local_sem.at[i])
        load.start()
        loads.append(load)
    l_order, l_rs, l_col, l_row, l_perm, l_diag = loads[:6]

    lane = lax.broadcasted_iota(jnp.int32, (SIDES, LANES), 1)
    zero = jnp.zeros((SIDES, LANES), F32)

    def plane(turn):
        return lax.rem(z + turn, Z)

    def slot_of(values, place):
        tile, offset = divmod(place * RANK, LANES)
        piece = values[:, tile * LANES : (tile + 1) * LANES]
        if offset + RANK > LANES:
            piece = jnp.where(lane >= offset, piece, values[:, (tile + 1) * LANES : (tile + 2) * LANES])
        return pltpu.roll(piece, LANES - offset, 1) if offset else piece

    def leaf_send(apply, n, out, into, send, recv, q):
        pltpu.make_async_remote_copy(
            src_ref=out.at[apply, n], dst_ref=into.at[apply, leaf],
            send_sem=send.at[apply], recv_sem=recv, device_id={"leaf": q}, device_id_type=MESH,
        ).start()

    def put_slots(base, values, extra):
        for i in range(X if values.shape[1] == 2 * LANES else LEAVES):
            slots[base + i] = jnp.where(lane < RANK, slot_of(values, i), extra)

    def send_peers(apply, turns, out, into, send, recv):
        for n, (dz, dx) in enumerate(LEAF_STEPS):
            if dz in turns:
                q = leaf_peers[n]
                out[apply, n] = slots[q].astype(BF16)
                leaf_send(apply, n, out, into, send, recv.at[apply, int(dz in FAR_TURNS)], q)

    def leaf_wait(apply, count, into, send, recv):
        part = into.at[apply, pl.ds(0, count)]
        pltpu.make_async_remote_copy(
            src_ref=part, dst_ref=part, send_sem=send.at[apply], recv_sem=recv,
            device_id={"leaf": leaf_peers[0]}, device_id_type=MESH,
        ).wait_recv()

    def joined(apply, turn, into):
        tiles = [None, None]

        def put(tile, value):
            tiles[tile] = value if tiles[tile] is None else tiles[tile] + value

        base = plane(turn) * X
        for i in range(X):
            tile, offset = divmod(i * RANK, LANES)
            value = jnp.where(lane < RANK, into[apply, base + i].astype(F32), 0.0)
            if offset:
                value = pltpu.roll(value, offset, 1)
            if offset + RANK > LANES:
                put(tile, jnp.where(lane >= offset, value, 0.0))
                put(tile + 1, jnp.where(lane < offset, value, 0.0))
            else:
                put(tile, value)
        return jnp.concatenate(tiles, axis=1).astype(BF16)[:, :PLANE]

    def received(apply, turns, into, factor):
        total = None
        for turn in turns:
            product = nn_dot(joined(apply, turn, into), factor[plane(turn)])
            total = product if total is None else total + product
        return total

    def rows_copy(src, dst, sems, r):
        return pltpu.make_async_remote_copy(
            src_ref=src, dst_ref=dst, send_sem=sems.at[0], recv_sem=sems.at[1],
            device_id={"rows": r}, device_id_type=MESH,
        )

    def rows_wait(into, sems):
        part = into.at[pl.ds(0, ROWB - 1)]
        return rows_copy(part, part, sems, row_peers[0])

    def summed(into):
        total = into[0]
        for r in range(1, ROWB):
            total = total + into[r]
        return total

    def side_sum(products):
        return jnp.sum(products, axis=1, keepdims=True)

    def to_points(values):
        parts = [nt_dot(part, onehot[...]) for part in three_parts(values)]
        return (parts[0] + parts[1]) + parts[2]

    l_order.wait()
    local_index = order[...] % PTS
    step = 128
    for start in range(0, PTS, step):
        point = lax.broadcasted_iota(jnp.int32, (step, PTS), 0) + start
        onehot[pl.ds(start, step), :] = jnp.where(point == local_index, 1.0, 0.0).astype(BF16)
    l_rs.wait()
    rs_high, rs_middle, rs_low = three_parts(rs[...])
    tree_high = nn_dot(rs_high, onehot[...])
    l_col.wait()
    values = nn_dot(tree_high.astype(BF16), col[...])
    for g in range(LEAVES):
        tile, offset = divmod(g * RANK, LANES)
        piece = values[:, tile * LANES : (tile + 1) * LANES]
        if offset + RANK > LANES:
            piece = jnp.where(lane >= offset, piece, values[:, (tile + 1) * LANES : (tile + 2) * LANES])
        if offset:
            piece = pltpu.roll(piece, LANES - offset, 1)
        first_slots[g] = jnp.where(lane < RANK, piece, 0.0)
    l_perm.wait()
    l_row.wait()
    pl.semaphore_wait(barrier, len(LEAF_STEPS) + len(ROW_STEPS))
    for n, q in enumerate(leaf_peers):
        a_out[0, n] = first_slots[perm[q]].astype(BF16)
        leaf_send(0, n, a_out, a_in, a_send, a_recv.at[0, int(LEAF_STEPS[n][0] in FAR_TURNS)], q)
    a_in[0, leaf] = first_slots[perm[leaf]].astype(BF16)

    @pl.when(leaf >= 0)
    def _():
        gram = nt_dot(row_factor[...], row_factor[...])
        own_gram[...] = jnp.concatenate([gram, jnp.zeros((RANK, LANES - RANK), F32)], axis=1)
        for r in row_peers:
            rows_copy(own_gram, gram_in.at[row], gram_sems, r).start()
        gram_in[row] = own_gram[...]

    @pl.when(leaf >= 0)
    def _():
        tree_middle = nn_dot(jnp.concatenate([rs_middle, rs_low], axis=0), onehot[...])
        field[0] = (tree_high + tree_middle[:SIDES]) + tree_middle[SIDES:]
        for t in range(LEAVES * RANK // LANES):
            turned = col[:, t * LANES : (t + 1) * LANES].T
            start = 0
            while start < LANES:
                g, first = divmod(t * LANES + start, RANK)
                count = min(RANK - first, LANES - start)
                col_t[g, pl.ds(first, count), :] = turned[start : start + count]
                start += count
        for q in range(LEAVES):
            p, i = divmod(q, X)
            back_q[0, p, pl.ds(i * RANK, RANK), :] = col_t[perm[q]]
        l_diag.wait()
        diag_points = jnp.broadcast_to(diag[...], (SIDES, PTS))
        diag_tree = [nn_dot(part, onehot[...]) for part in three_parts(diag_points)]
        diag_tree = (diag_tree[0] + diag_tree[1]) + diag_tree[2]
        scale[0] = 1.0 / diag_tree
        scale[1] = diag_tree
        for load in loads[6:]:
            load.wait()


    def build_gram():
        rows_wait(gram_in, gram_sems).wait_recv()
        wide = lax.broadcasted_iota(jnp.int32, (RANK, LANES), 1)
        for j in range(ROWB):
            tile, offset = divmod(j * RANK, LANES)
            value = gram_in[j]
            if offset:
                value = pltpu.roll(value, offset, 1)
            parts = [jnp.zeros((RANK, LANES), F32)] * TILES
            if offset + RANK > LANES:
                parts[tile] = jnp.where(wide >= offset, value, 0.0)
                parts[tile + 1] = jnp.where(wide < offset, value, 0.0)
            else:
                parts[tile] = value
            whole = jnp.concatenate(parts, axis=1)
            high = whole.astype(BF16)
            gram_high[pl.ds(j * RANK, RANK), :] = high
            gram_low[pl.ds(j * RANK, RANK), :] = (whole - high.astype(F32)).astype(BF16)

    def build_returner(kind):
        for pair in range(Z // 2):
            rows = jnp.concatenate([weight[kind, 2 * pair], weight[kind, 2 * pair + 1]], axis=0)
            product = nt_dot(gram_high[...], rows) + nt_dot(gram_low[...], rows)
            returner[kind, :, pair * GROUP : (pair + 1) * GROUP] = product.astype(BF16)

    def build_last(planes):
        for p in planes:
            back_q[1, p] = nt_dot(back_q[0, p], onehot[...]).astype(BF16)

    earlier_head = None
    dots_total = None
    for apply in range(APPLIES):
        kind, last = apply % 2, apply == APPLIES - 1
        @pl.when(leaf >= 0)
        def _():
            if 0 < apply:
                points[apply] = to_points(field[apply])
            if last:
                r0, z0, w0, y, d = field[0], field[1], field[2], field[3], scale[1]
                out = zero
                for i, products in enumerate([r0 * z0, z0 * w0, r0 * y, w0 * y, d * z0 * y, d * y * y]):
                    out = jnp.where(lane == i, side_sum(products), out)
                dots_out[...] = out
                for r in row_peers:
                    rows_copy(dots_out, dots_in.at[row], dots_sems, r).start()
                dots_in[row] = out

        leaf_wait(apply, NEAR_COUNT, a_in, a_send, a_recv.at[apply, 0])
        partial = received(apply, NEAR_TURNS, a_in, weight.at[kind])
        leaf_wait(apply, FAR_COUNT, a_in, a_send, a_recv.at[apply, 1])
        partial = partial + received(apply, FAR_TURNS, a_in, weight.at[kind])
        b_out[apply] = partial
        for r in row_peers:
            rows_copy(b_out.at[apply], b_in.at[apply, row], b_sems.at[apply], r).start()
        b_in[apply, row] = partial
        @pl.when(leaf >= 0)
        def _():
            if apply == 0:
                build_gram()
                build_returner(0)
            if last:
                rows_wait(dots_in, dots_sems).wait_recv()
                dots_sum[...] = summed(dots_in)

        rows_wait(b_in.at[apply], b_sems.at[apply]).wait_recv()
        head = summed(b_in.at[apply]).astype(BF16)
        extra = zero
        if apply == 1:
            earlier_head = head.astype(F32)
        if last:
            back = nn_dot(head, gram_high[...]) + nn_dot(head, gram_low[...])
            dots = jnp.where(lane == 6, side_sum(earlier_head * back), dots_sum[...])
            dots = jnp.where(lane == 7, side_sum(head.astype(F32) * back), dots)
            high, middle, low = three_parts(dots)
            extra = (
                pltpu.roll(high.astype(F32), 64, 1)
                + pltpu.roll(middle.astype(F32), 72, 1)
                + pltpu.roll(low.astype(F32), 80, 1)
            )
        put_slots(0, nn_dot(head, returner[kind]), extra)
        send_peers(apply, FAR_TURNS + NEAR_TURNS, c_out, c_in, c_send, c_recv)
        c_in[apply, leaf] = slots[leaf].astype(BF16)
        @pl.when(leaf >= 0)
        def _():
            if apply == 0:
                for p in range(Z):
                    col_q[p] = back_q[0, p].T
                build_returner(1)
            if apply in (1, 2):
                build_last(range(4) if apply == 1 else range(4, 8))

        factor = back_q.at[int(last)]
        leaf_wait(apply, NEAR_COUNT, c_in, c_send, c_recv.at[apply, 0])
        image = received(apply, NEAR_TURNS, c_in, factor)
        if last:
            for q in [plane(turn) * X + i for turn in NEAR_TURNS for i in range(X)]:
                value = c_in[apply, q].astype(F32)
                dots_total = value if dots_total is None else dots_total + value
        leaf_wait(apply, FAR_COUNT, c_in, c_send, c_recv.at[apply, 1])
        image = image + received(apply, FAR_TURNS, c_in, factor)
        if last:
            for q in [plane(turn) * X + i for turn in FAR_TURNS for i in range(X)]:
                dots_total = dots_total + c_in[apply, q].astype(F32)
        if not last:
            following = scale[kind] * field[apply] + image
            field[apply + 1] = following
            taken = following.astype(BF16)
            for turns in (FAR_TURNS, NEAR_TURNS):
                for turn in turns:
                    values = nn_dot(taken, col_q[plane(turn)])
                    values = jnp.concatenate([values, jnp.zeros((SIDES, 2 * LANES - PLANE), F32)], axis=1)
                    put_slots(plane(turn) * X, values, zero)
                send_peers(apply + 1, turns, a_out, a_in, a_send, a_recv)
            a_in[apply + 1, leaf] = slots[leaf].astype(BF16)

    def dot_value(i):
        return (
            dots_total[:, 64 + i : 65 + i] + dots_total[:, 72 + i : 73 + i] + dots_total[:, 80 + i : 81 + i]
        )

    rz, zw, ry, wy = (dot_value(i) for i in range(4))
    zt, yt = dot_value(4) + dot_value(6), dot_value(5) + dot_value(7)
    alpha = rz / zw
    rz_next = (rz - alpha * zw) - alpha * (ry - alpha * wy)
    along = 1.0 + rz_next / rz
    alpha_next = rz_next / (along * along * zw - along * alpha * (zt + wy) + alpha * alpha * yt)
    z0, w0, y = points[1], points[2], points[3]
    t = diag[...] * y + image
    x1_ref[...] = alpha * z0
    p1_ref[...] = along * z0 - alpha * y
    r1_ref[...] = rs[...] - alpha * w0
    image_ref[...] = along * w0 - alpha * t
    alpha_ref[...] = jnp.broadcast_to(alpha_next, (SIDES, PTS))

    for r in row_peers:
        rows_copy(own_gram, gram_in.at[row], gram_sems, r).wait_send()
        rows_copy(dots_out, dots_in.at[row], dots_sems, r).wait_send()
    for apply in range(APPLIES):
        for out, send in ((a_out, a_send), (c_out, c_send)):
            pltpu.make_async_remote_copy(
                src_ref=out.at[apply], dst_ref=out.at[apply],
                send_sem=send.at[apply], recv_sem=a_recv.at[apply, 0],
                device_id={"leaf": leaf_peers[0]}, device_id_type=MESH,
            ).wait_send()
        for r in row_peers:
            rows_copy(b_out.at[apply], b_in.at[apply, row], b_sems.at[apply], r).wait_send()


def per_device(
    right_side, diagonal, tree_order, mid_perm, col_factor, mid_factor, pre_factor, row_factor
):
    hbm = pl.BlockSpec(memory_space=pl.ANY)
    vmem = pl.BlockSpec(memory_space=pltpu.VMEM)
    diagonal, tree_order = diagonal.reshape(1, PTS), tree_order.reshape(1, PTS)
    mid_factor, pre_factor = mid_factor.reshape(Z, PLANE, GROUP), pre_factor.reshape(Z, PLANE, GROUP)
    right_side, diagonal, tree_order, mid_perm, col_factor, mid_factor, pre_factor, row_factor = (
        pltpu.with_memory_space_constraint(array, pltpu.HBM)
        for array in (right_side, diagonal, tree_order, mid_perm, col_factor, mid_factor, pre_factor, row_factor)
    )
    x1, p1, r1, image, alpha = pl.pallas_call(
        kernel,
        out_shape=(jax.ShapeDtypeStruct((SIDES, PTS), F32),) * 5,
        in_specs=[hbm] * 8,
        out_specs=(vmem,) * 5,
        scratch_shapes=[
            pltpu.VMEM((SIDES, PTS), F32),
            pltpu.VMEM((1, PTS), F32),
            pltpu.VMEM((1, PTS), jnp.int32),
            pltpu.SMEM((LEAVES,), jnp.int32),
            pltpu.VMEM((PTS, LEAVES * RANK), BF16),
            pltpu.VMEM((LEAVES, RANK, PTS), BF16),
            pltpu.VMEM((Z, PTS, PLANE), BF16),
            pltpu.VMEM((2, Z, PLANE, PTS), BF16),
            pltpu.VMEM((2, Z, PLANE, GROUP), BF16),
            pltpu.VMEM((2, GROUP, LEAVES * RANK), BF16),
            pltpu.VMEM((RANK, PTS), BF16),
            pltpu.VMEM((PTS, PTS), BF16),
            pltpu.VMEM((APPLIES, SIDES, PTS), F32),
            pltpu.VMEM((2, SIDES, PTS), F32),
            pltpu.VMEM((APPLIES, SIDES, PTS), F32),
            pltpu.VMEM((LEAVES, SIDES, LANES), F32),
            pltpu.VMEM((LEAVES, SIDES, LANES), F32),
            pltpu.VMEM((RANK, LANES), F32),
            pltpu.VMEM((ROWB, RANK, LANES), F32),
            pltpu.VMEM((GROUP, GROUP), BF16),
            pltpu.VMEM((GROUP, GROUP), BF16),
            pltpu.VMEM((SIDES, LANES), F32),
            pltpu.VMEM((ROWB, SIDES, LANES), F32),
            pltpu.VMEM((SIDES, LANES), F32),
            pltpu.VMEM((APPLIES, LEAVES - 1, SIDES, LANES), BF16),
            pltpu.VMEM((APPLIES, LEAVES, SIDES, LANES), BF16),
            pltpu.VMEM((APPLIES, SIDES, GROUP), F32),
            pltpu.VMEM((APPLIES, ROWB, SIDES, GROUP), F32),
            pltpu.VMEM((APPLIES, LEAVES - 1, SIDES, LANES), BF16),
            pltpu.VMEM((APPLIES, LEAVES, SIDES, LANES), BF16),
            pltpu.SemaphoreType.DMA((8,)),
            pltpu.SemaphoreType.DMA((2,)),
            pltpu.SemaphoreType.DMA((2,)),
            pltpu.SemaphoreType.DMA((APPLIES,)),
            pltpu.SemaphoreType.DMA((APPLIES, 2)),
            pltpu.SemaphoreType.DMA((APPLIES, 2)),
            pltpu.SemaphoreType.DMA((APPLIES,)),
            pltpu.SemaphoreType.DMA((APPLIES, 2)),
        ],
        compiler_params=pltpu.CompilerParams(
            collective_id=0, has_side_effects=True, vmem_limit_bytes=40000 * 1024
        ),
    )(
        right_side, diagonal, tree_order, mid_perm,
        col_factor, mid_factor, pre_factor, row_factor,
    )
    return x1 + alpha * p1, r1 - alpha * image


def solution(mesh):
    every = ("leaf", "rows")
    return jax.shard_map(
        per_device,
        mesh=mesh,
        in_specs=(
            P(None, every), P(every), P(every), P(),
            P(every, None), P("leaf", "rows"), P("leaf", "rows"), P(None, every),
        ),
        out_specs=(P(None, every), P(None, every)),
        check_vma=False,
    )
```
